32 devices in a mesh: rays: 2 (over x), freq: 16 (over z, y, core).
Axes of the slice: x: 2, y: 2, z: 4, core: 2. Of those that a mesh axis runs over, the one named last changes fastest.
Arguments:
- spectra: bfloat16 [32, 2, 1024, 1024], P(('rays', 'freq')), parts along dimension 0, may hold values from -6 to 6
- wavelet: float32 [16, 2], P('freq'), may hold values from -6 to 6
- freq_index: int32 [16], P('freq'), may hold values from 0 to 15, each once
- slowness: float32 [16], replicated, may hold values from 0.000222 to 0.000667
- layer_ids: int32 [1], replicated, may hold values from 0 to 15
- ray_slowness: float32 [4], P('rays'), parts along dimension 0, may hold values from -0.0001 to 0.0001
Outputs:
- migrated_image: float32 [2, 1024, 1024], P('rays', 'freq'), parts along dimension 0
The draws below stay inside these ranges and needn't reach their ends.
There are 2 independent parts, one for each index of `rays`. The reference program is written for one: setup_inputs(seed, part) draws one part's arguments, and reference() takes and returns one part's arrays. A program takes and returns all parts, laid end to end along the dimension named above; an argument that names none is the same for every part. Nothing has to cross between parts.
Inputs may be any that keep to these rules, and one draw needn't show every extreme that they name: `freq_index`: each frequency 0 to 15 is held by exactly one slot.
All inputs are finite; a program needn't handle non-finite values.
Results may differ from the reference program's by a relative error of at most 0.0065.
Values sent between devices are 32-bit elements; how exact they have to be, the bound alone decides.
A program may use at most 128 MiB of HBM per device.

```python
import math
import jax
import jax.numpy as jnp
from jax import lax

NX = 1024
NY = 1024
DEPTHS = 1
LAYERS = 16
FREQS = 16


def levels(own_key, extent, shards, smallest, high):
    gain = 1.0
    for dim, parts in shards:
        heights = jax.random.uniform(jax.random.fold_in(jax.random.fold_in(own_key, 6), dim), (parts,), jnp.float32, smallest / len(shards), high / len(shards))
        gain = gain * jnp.repeat(jnp.exp(heights), extent[dim] // parts).reshape((-1,) + (1,) * (len(extent) - 1 - dim))
    return gain


def normal_values(stream_key, extent, width, limit, pieces=(), kind=jnp.bfloat16):
    loudness = levels(stream_key, extent, pieces, -0.22, 0.18) if pieces else 1.0
    drawn = jax.random.normal(stream_key, extent, jnp.float32) * width * loudness
    return jnp.minimum(jnp.maximum(drawn, -limit), limit).astype(kind)


def setup_inputs(seed: int = 0, part: int = 0) -> dict:
    streams_of = jax.random.split(jax.random.key(seed), 7)
    own_keys = jax.random.split(jax.random.fold_in(streams_of[6], part), 7)
    spectra = normal_values(own_keys[0], (FREQS, 2, NY, NX), 1.0, 6.0, ((0, 16),))
    wavelet = normal_values(streams_of[1], (FREQS, 2), 1.0, 6.0, ((0, 16),), jnp.float32)
    freq_index = jax.random.permutation(streams_of[2], FREQS).astype(jnp.int32)
    slowness = jnp.clip(jnp.exp(jax.random.uniform(streams_of[3], (LAYERS,), jnp.float32, math.log(0.000222), math.log(0.000667))), 0.000222, 0.000667)
    layer_ids = jax.random.randint(streams_of[4], (DEPTHS,), 0, LAYERS).astype(jnp.int32)
    ray_slowness = jnp.clip(jax.random.uniform(own_keys[5], (2,), jnp.float32, -0.0001, 0.0001), -0.0001, 0.0001)
    return {"spectra": spectra, "wavelet": wavelet, "freq_index": freq_index, "slowness": slowness, "layer_ids": layer_ids, "ray_slowness": ray_slowness}


GRID_STEP = 12.5
DEPTH_STEP = 10.0
LOW_FREQUENCY = 5.0
FREQUENCY_BAND = 50.0
DAMPING = 6.0
radix_factor = 8

def block_table(length):
    left_side = jnp.arange(length, dtype=jnp.int32)[:, None]
    right_side = jnp.arange(length, dtype=jnp.int32)[None, :]
    angles = (left_side * right_side % length).astype(jnp.float32) * (2.0 * math.pi / length)
    cosines = jnp.cos(angles)
    sines = jnp.sin(angles)
    from_real = jnp.stack([cosines, sines], axis=1)
    from_imag = jnp.stack([-sines, cosines], axis=1)
    return jnp.stack([from_real, from_imag], axis=0).astype(jnp.bfloat16).astype(jnp.float32)

def twiddle(length):
    outer_pos = jnp.arange(radix_factor, dtype=jnp.int32)[:, None]
    inner_pos = jnp.arange(length // radix_factor, dtype=jnp.int32)[None, :]
    angles = (outer_pos * inner_pos % length).astype(jnp.float32) * (2.0 * math.pi / length)
    return (jnp.cos(angles), jnp.sin(angles))

def inverse_rows(field, small_table, large_table, twists):
    row_total = field.shape[1]
    column_total = field.shape[2]
    shaped = field.reshape(2, radix_factor, row_total // radix_factor, column_total).astype(jnp.float32)
    initial = jnp.einsum('cakx,cadn->dnkx', shaped, small_table, precision=lax.Precision.HIGHEST)
    cosines, sines = twists
    real_part = initial[0] * cosines[:, :, None] - initial[1] * sines[:, :, None]
    imag_part = initial[0] * sines[:, :, None] + initial[1] * cosines[:, :, None]
    turned = jnp.stack([real_part, imag_part]).astype(jnp.bfloat16).astype(jnp.float32)
    second = jnp.einsum('cnkx,ckdm->dmnx', turned, large_table, precision=lax.Precision.HIGHEST)
    return second.reshape(2, row_total, column_total).astype(jnp.bfloat16)

def inverse_columns(field, small_table, large_table, twists):
    row_total = field.shape[1]
    column_total = field.shape[2]
    shaped = field.reshape(2, row_total, radix_factor, column_total // radix_factor).astype(jnp.float32)
    initial = jnp.einsum('crak,cadn->drnk', shaped, small_table, precision=lax.Precision.HIGHEST)
    cosines, sines = twists
    real_part = initial[0] * cosines[None] - initial[1] * sines[None]
    imag_part = initial[0] * sines[None] + initial[1] * cosines[None]
    turned = jnp.stack([real_part, imag_part]).astype(jnp.bfloat16).astype(jnp.float32)
    second = jnp.einsum('crnk,ckdm->drmn', turned, large_table, precision=lax.Precision.HIGHEST)
    return second.reshape(2, row_total, column_total)

def wavenumbers(length):
    positions = jnp.arange(length, dtype=jnp.int32)
    signed = jnp.where(positions >= length // 2, positions - length, positions)
    return signed.astype(jnp.float32) * (2.0 * math.pi / (length * GRID_STEP))

def phase_factor(angular, layer_slow, wave_square):
    real_arg = (angular * angular - DAMPING * DAMPING) * layer_slow * layer_slow - wave_square
    imag_arg = 2.0 * angular * DAMPING * layer_slow * layer_slow
    modulus = jnp.sqrt(real_arg * real_arg + imag_arg * imag_arg)
    larger = jnp.sqrt(0.5 * (modulus + jnp.abs(real_arg)))
    smaller = imag_arg / (2.0 * larger)
    vertical_real = jnp.where(real_arg >= 0.0, larger, smaller)
    vertical_imag = jnp.where(real_arg >= 0.0, smaller, larger)
    damping_factor = jnp.exp(-vertical_imag * DEPTH_STEP)
    return (damping_factor * jnp.cos(vertical_real * DEPTH_STEP), damping_factor * jnp.sin(vertical_real * DEPTH_STEP))

def layer_value(slowness, layer_id):
    matches = jnp.arange(slowness.shape[0], dtype=jnp.int32) == layer_id
    return jnp.sum(jnp.where(matches, slowness, jnp.float32(0.0)))

def reference(spectra, wavelet, freq_index, slowness, layer_ids, ray_slowness):
    wave_y = wavenumbers(NY)
    wave_x = wavenumbers(NX)
    wave_square = wave_y[:, None] * wave_y[:, None] + wave_x[None, :] * wave_x[None, :]
    small_table = block_table(radix_factor)
    row_table = block_table(NY // radix_factor)
    column_table = block_table(NX // radix_factor)
    row_twists = twiddle(NY)
    column_twists = twiddle(NX)
    layer_slows = []
    delays = []
    delay_time = jnp.float32(0.0)
    for depth_level in range(DEPTHS):
        layer_slow = layer_value(slowness, layer_ids[depth_level])
        vertical = jnp.sqrt(layer_slow * layer_slow - ray_slowness[0] * ray_slowness[0] - ray_slowness[1] * ray_slowness[1])
        delay_time = delay_time + vertical * DEPTH_STEP
        layer_slows.append(layer_slow)
        delays.append(delay_time)
    column_place = jnp.arange(NX, dtype=jnp.int32).astype(jnp.float32) * GRID_STEP
    row_place = jnp.arange(NY, dtype=jnp.int32).astype(jnp.float32) * GRID_STEP

    def per_frequency(running, inputs):
        images, energies = running
        spectrum_in, wave_pair, position = inputs
        angular = (position.astype(jnp.float32) * (FREQUENCY_BAND / FREQS) + LOW_FREQUENCY) * (2.0 * math.pi)
        spectrum = spectrum_in.astype(jnp.float32)
        for depth_level in range(DEPTHS):
            cos_part, sin_part = phase_factor(angular, layer_slows[depth_level], wave_square)
            real_new = spectrum[0] * cos_part - spectrum[1] * sin_part
            imag_new = spectrum[0] * sin_part + spectrum[1] * cos_part
            spectrum = jnp.stack([real_new, imag_new])
            energies = energies.at[depth_level].add(jnp.sum(real_new * real_new + imag_new * imag_new))
            row_field = inverse_rows(spectrum.astype(jnp.bfloat16), small_table, row_table, row_twists)
            receiver = inverse_columns(row_field, small_table, column_table, column_twists)
            source_phase = angular * (ray_slowness[0] * column_place[None, :] + ray_slowness[1] * row_place[:, None] + delays[depth_level])
            cos_src = jnp.cos(source_phase)
            sin_src = jnp.sin(source_phase)
            weight_real = wave_pair[0] * cos_src + wave_pair[1] * sin_src
            weight_imag = wave_pair[0] * sin_src - wave_pair[1] * cos_src
            images = images.at[depth_level].add(weight_real * receiver[0] - weight_imag * receiver[1])
        return ((images, energies), None)
    start = (jnp.zeros((DEPTHS, NY, NX), jnp.float32), jnp.zeros((DEPTHS,), jnp.float32))
    (images, energies), unused = lax.scan(per_frequency, start, (spectra, wavelet, freq_index))
    energy_scale = 1.0 / jnp.sqrt(energies / FREQS + 1e-06)
    return images * energy_scale[:, None, None]
```

```python
import functools
import math

import jax
import jax.numpy as jnp
from jax import lax
from jax.experimental import pallas as pl
from jax.experimental.pallas import tpu as pltpu
from jax.sharding import PartitionSpec as P

GRID_STEP = 12.5
DEPTH_STEP = 10.0
LOW_FREQUENCY = 5.0
FREQUENCY_BAND = 50.0
DAMPING = 6.0
X_RADIX = 8
LANES = 128
MESH = pl.DeviceIdType.MESH

SIN_COEFS = [(-1.0) ** i / math.factorial(2 * i + 1) for i in range(6)]
COS_COEFS = [(-1.0) ** i / math.factorial(2 * i) for i in range(7)]


def half_sincos(half):
    square = half * half
    sine = jnp.full_like(square, SIN_COEFS[-1])
    for coef in SIN_COEFS[-2::-1]:
        sine = sine * square + coef
    sine = sine * half
    cosine = jnp.full_like(square, COS_COEFS[-1])
    for coef in COS_COEFS[-2::-1]:
        cosine = cosine * square + coef
    twice = sine + sine
    return twice * cosine, 1.0 - twice * sine


def turn_sincos(turns):
    reduced = turns - jnp.floor(turns + 0.5)
    return half_sincos(reduced * math.pi)


def butterfly(parts):
    count = len(parts)
    if count == 1:
        return parts
    even = butterfly(parts[0::2])
    odd = butterfly(parts[1::2])
    low, high = [], []
    for i in range(count // 2):
        er, ei = even[i]
        xr, xi = odd[i]
        if i == 0:
            tr, ti = xr, xi
        elif 4 * i == count:
            tr, ti = -xi, xr
        elif 8 * i == count:
            root = math.sqrt(0.5)
            tr, ti = (xr - xi) * root, (xr + xi) * root
        elif 8 * i == 3 * count:
            root = math.sqrt(0.5)
            tr, ti = (xr + xi) * -root, (xr - xi) * root
        else:
            c = math.cos(2 * math.pi * i / count)
            s = math.sin(2 * math.pi * i / count)
            tr, ti = xr * c - xi * s, xr * s + xi * c
        low.append((er + tr, ei + ti))
        high.append((er - tr, ei - ti))
    return low + high


def kernel(
    groups, radix, pieces,
    scal, spec_hbm, out_ref,
    spec, zed, ytab, field, xtab, vecs, image, core_in, pair_in, low_in, high_in, etile, eall,
    load_sem, core_s, core_r, pair_s, pair_r, low_s, low_r, high_s, high_r, e_s, e_r,
):
    rows = spec.shape[1] * spec.shape[2]
    cols = spec.shape[3]
    short = rows // radix
    lines = groups // 4
    me = lax.axis_index("freq")
    core = lax.rem(me, 2)
    pair = lax.rem(me // 2, 2)
    spot = me // 4
    core_peer = me + 1 - 2 * core
    pair_peer = me + 2 - 4 * pair

    barrier = pltpu.get_barrier_semaphore()

    def greet(i, carry):
        pl.semaphore_signal(
            barrier, inc=1, device_id={"freq": lax.rem(me + i, groups)}, device_id_type=MESH
        )
        return carry

    lax.fori_loop(1, groups, greet, 0)

    strips = short // 16
    tiles = cols // LANES

    def load(i):
        window = pl.ds(pl.multiple_of(i * 16, 16), 16)
        return pltpu.make_async_copy(
            spec_hbm.at[:, :, window, :], spec.at[:, :, window, :], load_sem.at[i]
        )

    def start_load(i, carry):
        load(i).start()
        return carry

    lax.fori_loop(0, strips, start_load, 0)

    real_base = scal[0]
    imag_arg = scal[1]
    turn_x = scal[2]
    turn_y = scal[3]
    turn_0 = scal[4]
    wave_re = scal[5]
    wave_im = scal[6]
    freq_total = scal[7]

    block = cols // X_RADIX
    place = lax.broadcasted_iota(jnp.int32, (X_RADIX, cols), 1)
    outer = lax.broadcasted_iota(jnp.int32, (X_RADIX, cols), 0)
    eighth = lax.rem(place * outer, X_RADIX).astype(jnp.float32) * (1.0 / X_RADIX)
    vec_sin, vec_cos = turn_sincos(eighth + place.astype(jnp.float32) * turn_x)
    vecs[0] = vec_cos
    vecs[1] = vec_sin

    def x_table(step, carry):
        strip = step // tiles
        tile = lax.rem(step, tiles)
        at = pl.ds(pl.multiple_of(tile * LANES, LANES), LANES)
        k = lax.broadcasted_iota(jnp.int32, (16, LANES), 0) + strip * 16
        x = lax.broadcasted_iota(jnp.int32, (16, LANES), 1) + tile * LANES
        turns = lax.rem(k * x, cols).astype(jnp.float32) * (1.0 / cols)
        sine, cosine = turn_sincos(turns)
        for k1 in range(X_RADIX):
            vc = vecs[0, k1 : k1 + 1, at]
            vs = vecs[1, k1 : k1 + 1, at]
            row = pl.ds(pl.multiple_of(strip * 16 + k1 * block, 16), 16)
            row_im = pl.ds(pl.multiple_of(strip * 16 + k1 * block + cols, 16), 16)
            xtab[row, at] = (cosine * vc - sine * vs).astype(jnp.bfloat16)
            xtab[row_im, at] = (-(cosine * vs) - sine * vc).astype(jnp.bfloat16)
        return carry

    lax.fori_loop(0, (block // 16) * tiles, x_table, 0)

    ytiles = short // LANES

    def y_table(step, carry):
        n1 = step // (strips * ytiles)
        strip = lax.rem(step // ytiles, strips)
        tile = lax.rem(step, ytiles)
        n2 = lax.broadcasted_iota(jnp.int32, (16, LANES), 0) + strip * 16
        k2 = lax.broadcasted_iota(jnp.int32, (16, LANES), 1) + tile * LANES
        n = n2 * radix + n1
        turns = lax.rem(k2 * n, rows).astype(jnp.float32) * (1.0 / rows)
        sine, cosine = turn_sincos(turns + n.astype(jnp.float32) * turn_y + turn_0)
        real = (wave_re * cosine + wave_im * sine).astype(jnp.bfloat16)
        imag_f = wave_re * sine - wave_im * cosine
        imag = imag_f.astype(jnp.bfloat16)
        top = pl.ds(pl.multiple_of(strip * 16, 16), 16)
        bottom = pl.ds(pl.multiple_of(strip * 16 + short, 16), 16)
        left = pl.ds(pl.multiple_of(tile * LANES, LANES), LANES)
        right = pl.ds(pl.multiple_of(tile * LANES + short, LANES), LANES)
        ytab[n1, top, left] = real
        ytab[n1, top, right] = (-imag_f).astype(jnp.bfloat16)
        ytab[n1, bottom, left] = imag
        ytab[n1, bottom, right] = real
        return carry

    lax.fori_loop(0, radix * strips * ytiles, y_table, 0)

    step_y = 2.0 * math.pi / (rows * GRID_STEP)
    step_x = 2.0 * math.pi / (cols * GRID_STEP)
    imag_sq = imag_arg * imag_arg
    imag_half = imag_arg * 0.5

    def shift(strip, total):
        load(strip).wait()
        rows_at = pl.ds(pl.multiple_of(strip * 16, 16), 16)

        def inner(tile, acc):
            at = pl.ds(pl.multiple_of(tile * LANES, LANES), LANES)
            kx = lax.broadcasted_iota(jnp.int32, (16, LANES), 1) + tile * LANES
            kx = jnp.where(kx >= cols // 2, kx - cols, kx).astype(jnp.float32) * step_x
            base = real_base - kx * kx
            sub = lax.broadcasted_iota(jnp.int32, (16, LANES), 0) + strip * 16
            parts = []
            for k1 in range(radix):
                offset = k1 * short - (rows if k1 >= radix // 2 else 0)
                ky = (sub + offset).astype(jnp.float32) * step_y
                a = base - ky * ky
                m = a * a + imag_sq
                q = 0.5 * (m * lax.rsqrt(m) + jnp.abs(a))
                iq = lax.rsqrt(q)
                g = q * iq
                h = imag_half * iq
                forward = a >= 0.0
                vert_re = jnp.where(forward, g, h)
                vert_im = jnp.where(forward, h, g)
                damp = jnp.exp(vert_im * -DEPTH_STEP)
                sine, cosine = half_sincos(vert_re * (0.5 * DEPTH_STEP))
                cosine = cosine * damp
                sine = sine * damp
                re = spec[0, k1, rows_at, at].astype(jnp.float32)
                im = spec[1, k1, rows_at, at].astype(jnp.float32)
                new_re = re * cosine - im * sine
                new_im = re * sine + im * cosine
                acc = acc + (new_re * new_re + new_im * new_im)
                parts.append((new_re, new_im))
            for n1, (re, im) in enumerate(butterfly(parts)):
                zed[n1, rows_at, at] = re.astype(jnp.bfloat16)
                low = pl.ds(pl.multiple_of(strip * 16 + short, 16), 16)
                zed[n1, low, at] = im.astype(jnp.bfloat16)
            return acc

        return lax.fori_loop(0, tiles, inner, total)

    energy = lax.fori_loop(0, strips, shift, jnp.zeros((16, LANES), jnp.float32))
    etile[...] = energy[:8] + energy[8:]

    chips = groups // 2

    def y_stage(n1, carry):
        for part in range(cols // 256):
            at = slice(part * 256, part * 256 + 256)
            at_im = slice(cols + part * 256, cols + part * 256 + 256)
            res = jnp.dot(ytab[n1], zed[n1, :, at], preferred_element_type=jnp.float32)
            res = res.astype(jnp.bfloat16)
            field[:, n1, :, at] = res[:short].reshape(chips, 16, 256)
            field[:, n1, :, at_im] = res[short:].reshape(chips, 16, 256)
        return carry

    lax.fori_loop(0, radix, y_stage, 0)

    pl.semaphore_wait(barrier, groups - 1)

    def energy_copy(i):
        return pltpu.make_async_remote_copy(
            src_ref=etile, dst_ref=eall.at[i], send_sem=e_s.at[i], recv_sem=e_r.at[i],
            device_id={"freq": lax.rem(me + i, groups)}, device_id_type=MESH,
        )

    def energy_start(i, carry):
        energy_copy(i).start()
        return carry

    lax.fori_loop(1, groups, energy_start, 0)

    def order(j):
        half = j // 2
        return jnp.where(lax.rem(j, 2) == 0, half, lines - 1 - half)

    def core_copy(a, b):
        return pltpu.make_async_remote_copy(
            src_ref=image.at[a, b, 1 - core], dst_ref=core_in.at[a, b],
            send_sem=core_s.at[a, b], recv_sem=core_r.at[a, b],
            device_id={"freq": core_peer}, device_id_type=MESH,
        )

    size = radix // pieces

    def pair_copy(a, p):
        cut = pl.ds(p * size, size)
        return pltpu.make_async_remote_copy(
            src_ref=image.at[a, 1 - pair, core, cut], dst_ref=pair_in.at[a, cut],
            send_sem=pair_s.at[a, p], recv_sem=pair_r.at[a, p],
            device_id={"freq": pair_peer}, device_id_type=MESH,
        )

    def low_copy(a, p):
        cut = pl.ds(p * size, size)
        return pltpu.make_async_remote_copy(
            src_ref=image.at[a, pair, core, cut], dst_ref=low_in.at[a, cut],
            send_sem=low_s.at[a, p], recv_sem=low_r.at[a, p],
            device_id={"freq": jnp.minimum(spot + 1, lines - 1) * 4 + pair * 2 + core},
            device_id_type=MESH,
        )

    def high_copy(a, p):
        cut = pl.ds(p * size, size)
        return pltpu.make_async_remote_copy(
            src_ref=image.at[a, pair, core, cut], dst_ref=high_in.at[a, cut],
            send_sem=high_s.at[a, p], recv_sem=high_r.at[a, p],
            device_id={"freq": jnp.maximum(spot - 1, 0) * 4 + pair * 2 + core},
            device_id_type=MESH,
        )

    def second(a):
        core_copy(a, 1 - pair).wait_recv()
        for p in range(pieces):
            cut = pl.ds(p * size, size)
            image[a, 1 - pair, core, cut] = (
                image[a, 1 - pair, core, cut] + core_in[a, 1 - pair, cut]
            )
            pair_copy(a, p).start()

    def compute(j, carry):
        a = order(j)
        lhs = field[pl.ds(2 * a, 2)].reshape(2 * radix * 16, 2 * cols)
        for part in range(cols // 256):
            at = slice(part * 256, part * 256 + 256)
            res = jnp.dot(lhs, xtab[:, at], preferred_element_type=jnp.float32)
            res = res.reshape(2, radix, 2, 8, 256)
            for c in range(2):
                image[a, :, c, :, :, at] = res[:, :, c]
        core_copy(a, 1 - pair).start()
        core_copy(a, pair).start()

        @pl.when(j > 0)
        def _():
            second(order(jnp.maximum(j - 1, 0)))

        return carry

    lax.fori_loop(0, lines, compute, 0)
    second(order(lines - 1))

    def third(j, carry):
        a = order(j)
        core_copy(a, pair).wait_recv()

        def piece(p, inner):
            cut = pl.ds(p * size, size)
            pair_copy(a, p).wait_recv()
            image[a, pair, core, cut] = (
                image[a, pair, core, cut] + core_in[a, pair, cut] + pair_in[a, cut]
            )

            @pl.when(jnp.logical_and(a >= spot, spot > 0))
            def _():
                low_copy(a, p).wait_recv()
                image[a, pair, core, cut] = image[a, pair, core, cut] + low_in[a, cut]

            @pl.when(jnp.logical_and(a <= spot, spot < lines - 1))
            def _():
                high_copy(a, p).wait_recv()
                image[a, pair, core, cut] = image[a, pair, core, cut] + high_in[a, cut]

            @pl.when(a > spot)
            def _():
                low_copy(a, p).start()

            @pl.when(a < spot)
            def _():
                high_copy(a, p).start()

            return inner

        return lax.fori_loop(0, pieces, piece, carry)

    lax.fori_loop(0, lines, third, 0)

    def energy_take(i, total):
        energy_copy(i).wait_recv()
        return total + eall[i]

    total = lax.fori_loop(1, groups, energy_take, etile[...])
    total = jnp.sum(jnp.sum(total, axis=0, keepdims=True), axis=1, keepdims=True)
    scale = lax.rsqrt(total / freq_total + 1e-06)
    out_ref[...] = image[spot, pair, core] * scale.reshape(1, 1, 1)

    def energy_end(i, carry):
        energy_copy(i).wait_send()
        return carry

    lax.fori_loop(1, groups, energy_end, 0)

    def finish(a, carry):
        core_copy(a, 0).wait_send()
        core_copy(a, 1).wait_send()

        def piece(p, inner):
            pair_copy(a, p).wait_send()

            @pl.when(a > spot)
            def _():
                low_copy(a, p).wait_send()

            @pl.when(a < spot)
            def _():
                high_copy(a, p).wait_send()

            return inner

        return lax.fori_loop(0, pieces, piece, carry)

    lax.fori_loop(0, lines, finish, 0)


def body(spectra, wavelet, freq_index, slowness, layer_ids, ray_slowness):
    slot_total, unused, rows, cols = spectra.shape
    groups = lax.axis_size("freq")
    freq_total = slot_total * groups
    radix = rows // groups // 8
    short = rows // radix
    lines = groups // 4
    pieces = min(4, radix)
    hertz = freq_index[0].astype(jnp.float32) * (FREQUENCY_BAND / freq_total) + LOW_FREQUENCY
    angular = hertz * (2.0 * math.pi)
    matches = jnp.arange(slowness.shape[0], dtype=jnp.int32) == layer_ids[0]
    slow = jnp.sum(jnp.where(matches, slowness, jnp.float32(0.0)))
    ray_x, ray_y = ray_slowness[0], ray_slowness[1]
    delay = jnp.sqrt(slow * slow - ray_x * ray_x - ray_y * ray_y) * DEPTH_STEP
    scal = jnp.stack(
        [
            (angular * angular - DAMPING * DAMPING) * slow * slow,
            2.0 * angular * DAMPING * slow * slow,
            hertz * ray_x * GRID_STEP,
            hertz * ray_y * GRID_STEP,
            hertz * delay,
            wavelet[0, 0],
            wavelet[0, 1],
            jnp.float32(freq_total),
        ]
    )
    f32, bf16 = jnp.float32, jnp.bfloat16
    dma = pltpu.SemaphoreType.DMA
    out = pl.pallas_call(
        functools.partial(kernel, groups, radix, pieces),
        out_shape=jax.ShapeDtypeStruct((radix, 8, cols), f32),
        in_specs=[
            pl.BlockSpec(memory_space=pltpu.SMEM),
            pl.BlockSpec(memory_space=pl.ANY),
        ],
        out_specs=pl.BlockSpec(memory_space=pltpu.VMEM),
        scratch_shapes=[
            pltpu.VMEM((2, radix, short, cols), bf16),
            pltpu.VMEM((radix, 2 * short, cols), bf16),
            pltpu.VMEM((radix, 2 * short, 2 * short), bf16),
            pltpu.VMEM((groups // 2, radix, 16, 2 * cols), bf16),
            pltpu.VMEM((2 * cols, cols), bf16),
            pltpu.VMEM((2, X_RADIX, cols), f32),
            pltpu.VMEM((lines, 2, 2, radix, 8, cols), f32),
            pltpu.VMEM((lines, 2, radix, 8, cols), f32),
            pltpu.VMEM((lines, radix, 8, cols), f32),
            pltpu.VMEM((lines, radix, 8, cols), f32),
            pltpu.VMEM((lines, radix, 8, cols), f32),
            pltpu.VMEM((8, LANES), f32),
            pltpu.VMEM((groups, 8, LANES), f32),
            dma((short // 16,)),
            dma((lines, 2)),
            dma((lines, 2)),
            dma((lines, pieces)),
            dma((lines, pieces)),
            dma((lines, pieces)),
            dma((lines, pieces)),
            dma((lines, pieces)),
            dma((lines, pieces)),
            dma((groups,)),
            dma((groups,)),
        ],
        compiler_params=pltpu.CompilerParams(
            collective_id=0, has_side_effects=True, vmem_limit_bytes=60 * 1024 * 1024
        ),
    )(scal, spectra[0].reshape(2, radix, short, cols))
    return out.transpose(1, 0, 2).reshape(1, 8 * radix, cols)


def solution(mesh):
    placed = (
        P(("rays", "freq"), None, None, None),
        P("freq", None),
        P("freq"),
        P(),
        P(),
        P("rays"),
    )
    return jax.shard_map(
        body, mesh=mesh, in_specs=placed, out_specs=P("rays", "freq", None), check_vma=False
    )
```

```python
import functools
import math

import jax
import jax.numpy as jnp
from jax import lax
from jax.experimental import pallas as pl
from jax.experimental.pallas import tpu as pltpu
from jax.sharding import PartitionSpec as P

GRID_STEP = 12.5
DEPTH_STEP = 10.0
LOW_FREQUENCY = 5.0
FREQUENCY_BAND = 50.0
DAMPING = 6.0
X_RADIX = 8
LANES = 128
LAG = 2
DEPTH = 3
MESH = pl.DeviceIdType.MESH

SIN_COEFS = [(-1.0) ** i / math.factorial(2 * i + 1) for i in range(5)]
COS_COEFS = [(-1.0) ** i / math.factorial(2 * i) for i in range(6)]


def half_sincos(half):
    square = half * half
    sine = square * SIN_COEFS[-1] + SIN_COEFS[-2]
    for coef in SIN_COEFS[-3::-1]:
        sine = sine * square + coef
    sine = sine * half
    cosine = square * COS_COEFS[-1] + COS_COEFS[-2]
    for coef in COS_COEFS[-3::-1]:
        cosine = cosine * square + coef
    twice = sine + sine
    return twice * cosine, 1.0 - twice * sine


def turn_sincos(turns):
    reduced = turns - jnp.floor(turns + 0.5)
    return half_sincos(reduced * math.pi)


def butterfly(parts):
    count = len(parts)
    if count == 1:
        return parts
    even = butterfly(parts[0::2])
    odd = butterfly(parts[1::2])
    low, high = [], []
    for i in range(count // 2):
        er, ei = even[i]
        xr, xi = odd[i]
        if i == 0:
            tr, ti = xr, xi
        elif 4 * i == count:
            tr, ti = -xi, xr
        elif 8 * i == count:
            root = math.sqrt(0.5)
            tr, ti = (xr - xi) * root, (xr + xi) * root
        elif 8 * i == 3 * count:
            root = math.sqrt(0.5)
            tr, ti = (xr + xi) * -root, (xr - xi) * root
        else:
            c = math.cos(2 * math.pi * i / count)
            s = math.sin(2 * math.pi * i / count)
            tr, ti = xr * c - xi * s, xr * s + xi * c
        low.append((er + tr, ei + ti))
        high.append((er - tr, ei - ti))
    return low + high


def kernel(
    groups, radix, pieces, freq_total,
    wavelet, freq_index, slowness, layer_ids, rays, spec_hbm, out_ref,
    spec, zed, ytab, field, xtab, vecs, image, core_in, pair_in, low_in, high_in, etile, eall,
    load_sem, core_s, core_r, pair_s, pair_r, low_s, low_r, high_s, high_r, e_s, e_r,
):
    rows = spec.shape[1] * spec.shape[2]
    cols = spec.shape[3]
    short = rows // radix
    lines = groups // 4
    me = lax.axis_index("freq")
    core = lax.rem(me, 2)
    pair = lax.rem(me // 2, 2)
    spot = me // 4
    core_peer = me + 1 - 2 * core
    pair_peer = me + 2 - 4 * pair

    barrier = pltpu.get_barrier_semaphore()

    def greet(i, carry):
        pl.semaphore_signal(
            barrier, inc=1, device_id={"freq": lax.rem(me + i, groups)}, device_id_type=MESH
        )
        return carry

    lax.fori_loop(1, groups, greet, 0)

    strips = short // 16
    tiles = cols // LANES

    def load(i):
        window = pl.ds(pl.multiple_of(i * 16, 16), 16)
        return pltpu.make_async_copy(
            spec_hbm.at[:, :, window, :], spec.at[:, :, window, :], load_sem.at[i]
        )

    def start_load(i, carry):
        load(i).start()
        return carry

    lax.fori_loop(0, strips, start_load, 0)

    hertz = freq_index[0, 0].astype(jnp.float32) * (FREQUENCY_BAND / freq_total) + LOW_FREQUENCY
    angular = hertz * (2.0 * math.pi)
    slow = slowness[layer_ids[0, 0]]
    slow_sq = slow * slow
    ray_x = rays[0]
    ray_y = rays[1]
    real_base = (angular * angular - DAMPING * DAMPING) * slow_sq
    imag_arg = 2.0 * angular * DAMPING * slow_sq
    turn_x = hertz * ray_x * GRID_STEP
    turn_y = hertz * ray_y * GRID_STEP
    vertical = jnp.full((16, LANES), slow_sq - ray_x * ray_x - ray_y * ray_y, jnp.float32)
    turn_0 = jnp.sqrt(vertical) * (DEPTH_STEP * hertz)
    wave_re = wavelet[0, 0]
    wave_im = wavelet[0, 1]

    block = cols // X_RADIX
    place = lax.broadcasted_iota(jnp.int32, (X_RADIX, cols), 1)
    outer = lax.broadcasted_iota(jnp.int32, (X_RADIX, cols), 0)
    eighth = lax.rem(place * outer, X_RADIX).astype(jnp.float32) * (1.0 / X_RADIX)
    vec_sin, vec_cos = turn_sincos(eighth + place.astype(jnp.float32) * turn_x)
    vecs[0] = vec_cos
    vecs[1] = vec_sin

    def x_table(step, carry):
        strip = step // tiles
        tile = lax.rem(step, tiles)
        at = pl.ds(pl.multiple_of(tile * LANES, LANES), LANES)
        k = lax.broadcasted_iota(jnp.int32, (16, LANES), 0) + strip * 16
        x = lax.broadcasted_iota(jnp.int32, (16, LANES), 1) + tile * LANES
        turns = lax.rem(k * x, cols).astype(jnp.float32) * (1.0 / cols)
        sine, cosine = turn_sincos(turns)
        for k1 in range(X_RADIX):
            vc = vecs[0, k1 : k1 + 1, at]
            vs = vecs[1, k1 : k1 + 1, at]
            row = pl.ds(pl.multiple_of(strip * 16 + k1 * block, 16), 16)
            row_im = pl.ds(pl.multiple_of(strip * 16 + k1 * block + cols, 16), 16)
            xtab[row, at] = (cosine * vc - sine * vs).astype(jnp.bfloat16)
            xtab[row_im, at] = (-(cosine * vs) - sine * vc).astype(jnp.bfloat16)
        return carry

    lax.fori_loop(0, (block // 16) * tiles, x_table, 0)

    ytiles = short // LANES

    def y_table(step, carry):
        n1 = step // (strips * ytiles)
        strip = lax.rem(step // ytiles, strips)
        tile = lax.rem(step, ytiles)
        n2 = lax.broadcasted_iota(jnp.int32, (16, LANES), 0) + strip * 16
        k2 = lax.broadcasted_iota(jnp.int32, (16, LANES), 1) + tile * LANES
        n = n2 * radix + n1
        turns = lax.rem(k2 * n, rows).astype(jnp.float32) * (1.0 / rows)
        sine, cosine = turn_sincos(turns + n.astype(jnp.float32) * turn_y + turn_0)
        real = (wave_re * cosine + wave_im * sine).astype(jnp.bfloat16)
        imag_f = wave_re * sine - wave_im * cosine
        imag = imag_f.astype(jnp.bfloat16)
        top = pl.ds(pl.multiple_of(strip * 16, 16), 16)
        bottom = pl.ds(pl.multiple_of(strip * 16 + short, 16), 16)
        left = pl.ds(pl.multiple_of(tile * LANES, LANES), LANES)
        right = pl.ds(pl.multiple_of(tile * LANES + short, LANES), LANES)
        ytab[n1, top, left] = real
        ytab[n1, top, right] = (-imag_f).astype(jnp.bfloat16)
        ytab[n1, bottom, left] = imag
        ytab[n1, bottom, right] = real
        return carry

    lax.fori_loop(0, radix * strips * ytiles, y_table, 0)

    step_y = 2.0 * math.pi / (rows * GRID_STEP)
    step_x = 2.0 * math.pi / (cols * GRID_STEP)
    imag_sq = imag_arg * imag_arg
    imag_half = imag_arg * 0.5

    def shift(strip, total):
        load(strip).wait()
        rows_at = pl.ds(pl.multiple_of(strip * 16, 16), 16)

        def inner(tile, acc):
            at = pl.ds(pl.multiple_of(tile * LANES, LANES), LANES)
            kx = lax.broadcasted_iota(jnp.int32, (16, LANES), 1) + tile * LANES
            kx = jnp.where(kx >= cols // 2, kx - cols, kx).astype(jnp.float32) * step_x
            base = real_base - kx * kx
            sub = lax.broadcasted_iota(jnp.int32, (16, LANES), 0) + strip * 16
            parts = []
            for k1 in range(radix):
                offset = k1 * short - (rows if k1 >= radix // 2 else 0)
                ky = (sub + offset).astype(jnp.float32) * step_y
                a = base - ky * ky
                m = a * a + imag_sq
                q = 0.5 * (m * lax.rsqrt(m) + jnp.abs(a))
                iq = lax.rsqrt(q)
                g = q * iq
                h = imag_half * iq
                forward = a >= 0.0
                vert_re = jnp.where(forward, g, h)
                vert_im = jnp.where(forward, h, g)
                damp = jnp.exp(vert_im * -DEPTH_STEP)
                sine, cosine = half_sincos(vert_re * (0.5 * DEPTH_STEP))
                cosine = cosine * damp
                sine = sine * damp
                re = spec[0, k1, rows_at, at].astype(jnp.float32)
                im = spec[1, k1, rows_at, at].astype(jnp.float32)
                new_re = re * cosine - im * sine
                new_im = re * sine + im * cosine
                acc = acc + (new_re * new_re + new_im * new_im)
                parts.append((new_re, new_im))
            for n1, (re, im) in enumerate(butterfly(parts)):
                zed[n1, rows_at, at] = re.astype(jnp.bfloat16)
                low = pl.ds(pl.multiple_of(strip * 16 + short, 16), 16)
                zed[n1, low, at] = im.astype(jnp.bfloat16)
            return acc

        return lax.fori_loop(0, tiles, inner, total)

    energy = lax.fori_loop(0, strips, shift, jnp.zeros((16, LANES), jnp.float32))
    etile[...] = energy[:8] + energy[8:]

    chips = groups // 2

    def y_stage(n1, carry):
        for part in range(cols // 256):
            at = slice(part * 256, part * 256 + 256)
            at_im = slice(cols + part * 256, cols + part * 256 + 256)
            res = jnp.dot(ytab[n1], zed[n1, :, at], preferred_element_type=jnp.float32)
            res = res.astype(jnp.bfloat16)
            field[:, n1, :, at] = res[:short].reshape(chips, 16, 256)
            field[:, n1, :, at_im] = res[short:].reshape(chips, 16, 256)
        return carry

    lax.fori_loop(0, radix, y_stage, 0)

    pl.semaphore_wait(barrier, groups - 1)

    def energy_copy(i):
        return pltpu.make_async_remote_copy(
            src_ref=etile, dst_ref=eall.at[i], send_sem=e_s.at[i], recv_sem=e_r.at[i],
            device_id={"freq": lax.rem(me + i, groups)}, device_id_type=MESH,
        )

    def energy_start(i, carry):
        energy_copy(i).start()
        return carry

    lax.fori_loop(1, groups, energy_start, 0)

    def order(j):
        half = j // 2
        return jnp.where(lax.rem(j, 2) == 0, half, lines - 1 - half)

    def core_copy(a, b):
        return pltpu.make_async_remote_copy(
            src_ref=image.at[a, b, 1 - core], dst_ref=core_in.at[a, b],
            send_sem=core_s.at[a, b], recv_sem=core_r.at[a, b],
            device_id={"freq": core_peer}, device_id_type=MESH,
        )

    size = radix // pieces

    def pair_copy(a, p):
        cut = pl.ds(p * size, size)
        return pltpu.make_async_remote_copy(
            src_ref=image.at[a, 1 - pair, core, cut], dst_ref=pair_in.at[a, cut],
            send_sem=pair_s.at[a, p], recv_sem=pair_r.at[a, p],
            device_id={"freq": pair_peer}, device_id_type=MESH,
        )

    def low_copy(a, p):
        cut = pl.ds(p * size, size)
        return pltpu.make_async_remote_copy(
            src_ref=image.at[a, pair, core, cut], dst_ref=low_in.at[a, cut],
            send_sem=low_s.at[a, p], recv_sem=low_r.at[a, p],
            device_id={"freq": jnp.minimum(spot + 1, lines - 1) * 4 + pair * 2 + core},
            device_id_type=MESH,
        )

    def high_copy(a, p):
        cut = pl.ds(p * size, size)
        return pltpu.make_async_remote_copy(
            src_ref=image.at[a, pair, core, cut], dst_ref=high_in.at[a, cut],
            send_sem=high_s.at[a, p], recv_sem=high_r.at[a, p],
            device_id={"freq": jnp.maximum(spot - 1, 0) * 4 + pair * 2 + core},
            device_id_type=MESH,
        )

    count = lines * pieces
    depth = min(DEPTH, count)

    def split(i):
        return order(i // pieces), lax.rem(i, pieces)

    def send_pair(i):
        a, p = split(i)
        cut = pl.ds(p * size, size)

        @pl.when(p == 0)
        def _():
            core_copy(a, 1 - pair).wait_recv()

        image[a, 1 - pair, core, cut] = (
            image[a, 1 - pair, core, cut] + core_in[a, 1 - pair, cut]
        )
        pair_copy(a, p).start()

    def compute(j, carry):
        a = order(j)
        lhs = field[pl.ds(2 * a, 2)].reshape(2 * radix * 16, 2 * cols)
        for part in range(cols // 256):
            at = slice(part * 256, part * 256 + 256)
            res = jnp.dot(lhs, xtab[:, at], preferred_element_type=jnp.float32)
            res = res.reshape(2, radix, 2, 8, 256)
            for c in range(2):
                image[a, :, c, :, :, at] = res[:, :, c]
        core_copy(a, 1 - pair).start()
        core_copy(a, pair).start()

        @pl.when(j == min(1, lines - 1))
        def _():
            for i in range(depth):
                send_pair(i)

        return carry

    lax.fori_loop(0, lines, compute, 0)

    def third(i, carry):
        @pl.when(i < count)
        def _():
            a, p = split(jnp.minimum(i, count - 1))
            cut = pl.ds(p * size, size)
            pair_copy(a, p).wait_recv()

            @pl.when(i + depth < count)
            def _():
                send_pair(jnp.minimum(i + depth, count - 1))

            @pl.when(p == 0)
            def _():
                core_copy(a, pair).wait_recv()

            image[a, pair, core, cut] = (
                image[a, pair, core, cut] + core_in[a, pair, cut] + pair_in[a, cut]
            )

        upward = i - LAG * spot
        a_up, p_up = split(jnp.clip(upward, 0, count - 1))

        @pl.when((upward >= 0) & (upward < count) & (a_up > spot))
        def _():
            cut = pl.ds(p_up * size, size)

            @pl.when(spot > 0)
            def _():
                low_copy(a_up, p_up).wait_recv()
                image[a_up, pair, core, cut] = image[a_up, pair, core, cut] + low_in[a_up, cut]

            low_copy(a_up, p_up).start()

        downward = i - LAG * (lines - 1 - spot)
        a_dn, p_dn = split(jnp.clip(downward, 0, count - 1))

        @pl.when((downward >= 0) & (downward < count) & (a_dn < spot))
        def _():
            cut = pl.ds(p_dn * size, size)

            @pl.when(spot < lines - 1)
            def _():
                high_copy(a_dn, p_dn).wait_recv()
                image[a_dn, pair, core, cut] = image[a_dn, pair, core, cut] + high_in[a_dn, cut]

            high_copy(a_dn, p_dn).start()

        return carry

    lax.fori_loop(0, count + LAG * (lines - 1), third, 0)

    def energy_take(i, total):
        energy_copy(i).wait_recv()
        return total + eall[i]

    total = lax.fori_loop(1, groups, energy_take, etile[...])
    total = jnp.sum(jnp.sum(total, axis=0, keepdims=True), axis=1, keepdims=True)
    scale = lax.rsqrt(total / freq_total + 1e-06)

    def own(p, carry):
        cut = pl.ds(p * size, size)

        @pl.when(spot > 0)
        def _():
            low_copy(spot, p).wait_recv()
            image[spot, pair, core, cut] = image[spot, pair, core, cut] + low_in[spot, cut]

        @pl.when(spot < lines - 1)
        def _():
            high_copy(spot, p).wait_recv()
            image[spot, pair, core, cut] = image[spot, pair, core, cut] + high_in[spot, cut]

        return carry

    lax.fori_loop(0, pieces, own, 0)
    for n1 in range(radix):
        out_ref[:, n1, :] = image[spot, pair, core, n1] * scale

    def energy_end(i, carry):
        energy_copy(i).wait_send()
        return carry

    lax.fori_loop(1, groups, energy_end, 0)

    def finish(a, carry):
        core_copy(a, 0).wait_send()
        core_copy(a, 1).wait_send()

        def piece(p, inner):
            pair_copy(a, p).wait_send()

            @pl.when(a > spot)
            def _():
                low_copy(a, p).wait_send()

            @pl.when(a < spot)
            def _():
                high_copy(a, p).wait_send()

            return inner

        return lax.fori_loop(0, pieces, piece, carry)

    lax.fori_loop(0, lines, finish, 0)


def body(spectra, wavelet, freq_index, slowness, layer_ids, ray_slowness):
    slot_total, unused, rows, cols = spectra.shape
    groups = lax.axis_size("freq")
    freq_total = slot_total * groups
    radix = rows // groups // 8
    short = rows // radix
    lines = groups // 4
    pieces = min(4, radix)
    f32, bf16 = jnp.float32, jnp.bfloat16
    dma = pltpu.SemaphoreType.DMA
    out = pl.pallas_call(
        functools.partial(kernel, groups, radix, pieces, freq_total),
        out_shape=jax.ShapeDtypeStruct((8, radix, cols), f32),
        in_specs=[
            *[pl.BlockSpec(memory_space=pltpu.SMEM)] * 5,
            pl.BlockSpec(memory_space=pl.ANY),
        ],
        out_specs=pl.BlockSpec(memory_space=pltpu.VMEM),
        scratch_shapes=[
            pltpu.VMEM((2, radix, short, cols), bf16),
            pltpu.VMEM((radix, 2 * short, cols), bf16),
            pltpu.VMEM((radix, 2 * short, 2 * short), bf16),
            pltpu.VMEM((groups // 2, radix, 16, 2 * cols), bf16),
            pltpu.VMEM((2 * cols, cols), bf16),
            pltpu.VMEM((2, X_RADIX, cols), f32),
            pltpu.VMEM((lines, 2, 2, radix, 8, cols), f32),
            pltpu.VMEM((lines, 2, radix, 8, cols), f32),
            pltpu.VMEM((lines, radix, 8, cols), f32),
            pltpu.VMEM((lines, radix, 8, cols), f32),
            pltpu.VMEM((lines, radix, 8, cols), f32),
            pltpu.VMEM((8, LANES), f32),
            pltpu.VMEM((groups, 8, LANES), f32),
            dma((short // 16,)),
            dma((lines, 2)),
            dma((lines, 2)),
            dma((lines, pieces)),
            dma((lines, pieces)),
            dma((lines, pieces)),
            dma((lines, pieces)),
            dma((lines, pieces)),
            dma((lines, pieces)),
            dma((groups,)),
            dma((groups,)),
        ],
        compiler_params=pltpu.CompilerParams(
            collective_id=0, has_side_effects=True, vmem_limit_bytes=60 * 1024 * 1024
        ),
    )(
        wavelet, freq_index.reshape(1, 1), slowness, layer_ids.reshape(1, 1), ray_slowness,
        spectra.reshape(2, radix, short, cols),
    )
    return out.reshape(1, 8 * radix, cols)


def solution(mesh):
    placed = (
        P(("rays", "freq"), None, None, None),
        P("freq", None),
        P("freq"),
        P(),
        P(),
        P("rays"),
    )
    return jax.shard_map(
        body, mesh=mesh, in_specs=placed, out_specs=P("rays", "freq", None), check_vma=False
    )
```

```python
import functools
import math

import jax
import jax.numpy as jnp
from jax import lax
from jax.experimental import pallas as pl
from jax.experimental.pallas import tpu as pltpu
from jax.sharding import PartitionSpec as P

GRID_STEP = 12.5
DEPTH_STEP = 10.0
LOW_FREQUENCY = 5.0
FREQUENCY_BAND = 50.0
DAMPING = 6.0
X_RADIX = 8
LANES = 128
LAG = 2
DEPTH = 4
YTALL = 64
EARLY = 2
MESH = pl.DeviceIdType.MESH

PHASE_SIN = (0.9999998807907104, -0.16666465997695923, 0.008326363749802113, -0.00019062065985053778)
PHASE_COS = (0.9999992251396179, -0.499982088804245, 0.04160428047180176, -0.0013190462486818433)
TURN_SIN = (0.9999992251396179, -0.16665679216384888, 0.008313224650919437, -0.0001852344867074862)
TURN_COS = (
    0.9999999403953552, -0.4999990463256836, 0.041663579642772675, -0.0013853666605427861,
    2.315317397005856e-05,
)


def polynomial(coefs, square):
    value = square * coefs[-1] + coefs[-2]
    for coef in coefs[-3::-1]:
        value = value * square + coef
    return value


def half_sincos(half, sin_coefs, cos_coefs):
    square = half * half
    sine = polynomial(sin_coefs, square) * half
    twice = sine + sine
    return twice * polynomial(cos_coefs, square), 1.0 - twice * sine


def turn_sincos(turns):
    reduced = turns - jnp.floor(turns + 0.5)
    return half_sincos(reduced * math.pi, TURN_SIN, TURN_COS)


def butterfly(parts):
    count = len(parts)
    if count == 1:
        return parts
    even = butterfly(parts[0::2])
    odd = butterfly(parts[1::2])
    low, high = [], []
    for i in range(count // 2):
        er, ei = even[i]
        xr, xi = odd[i]
        if i == 0:
            tr, ti = xr, xi
        elif 4 * i == count:
            tr, ti = -xi, xr
        elif 8 * i == count:
            root = math.sqrt(0.5)
            tr, ti = (xr - xi) * root, (xr + xi) * root
        elif 8 * i == 3 * count:
            root = math.sqrt(0.5)
            tr, ti = (xr + xi) * -root, (xr - xi) * root
        else:
            c = math.cos(2 * math.pi * i / count)
            s = math.sin(2 * math.pi * i / count)
            tr, ti = xr * c - xi * s, xr * s + xi * c
        low.append((er + tr, ei + ti))
        high.append((er - tr, ei - ti))
    return low + high


def kernel(
    groups, radix, pieces, freq_total,
    wavelet, freq_index, slowness, layer_ids, rays, spec_hbm, out_ref,
    spec, zed, ytab, field, xtab, vecs, ybase, image, core_in, pair_in, low_in, high_in, etile, eall,
    load_sem, core_s, core_r, pair_s, pair_r, low_s, low_r, high_s, high_r, e_s, e_r,
):
    rows = spec.shape[1] * spec.shape[2]
    cols = spec.shape[3]
    short = rows // radix
    lines = groups // 4
    me = lax.axis_index("freq")
    core = lax.rem(me, 2)
    pair = lax.rem(me // 2, 2)
    spot = me // 4
    core_peer = me + 1 - 2 * core
    pair_peer = me + 2 - 4 * pair

    barrier = pltpu.get_barrier_semaphore()

    def greet(i, carry):
        pl.semaphore_signal(
            barrier, inc=1, device_id={"freq": lax.rem(me + i, groups)}, device_id_type=MESH
        )
        return carry

    lax.fori_loop(1, groups, greet, 0)

    strips = short // 16
    tiles = cols // LANES

    def load(i):
        window = pl.ds(pl.multiple_of(i * 16, 16), 16)
        return pltpu.make_async_copy(
            spec_hbm.at[:, :, window, :], spec.at[:, :, window, :], load_sem.at[i]
        )

    def start_load(i, carry):
        load(i).start()
        return carry

    lax.fori_loop(0, strips, start_load, 0)

    hertz = freq_index[0, 0].astype(jnp.float32) * (FREQUENCY_BAND / freq_total) + LOW_FREQUENCY
    angular = hertz * (2.0 * math.pi)
    slow = slowness[layer_ids[0, 0]]
    slow_sq = slow * slow
    ray_x = rays[0]
    ray_y = rays[1]
    real_base = (angular * angular - DAMPING * DAMPING) * slow_sq
    imag_arg = 2.0 * angular * DAMPING * slow_sq
    turn_x = hertz * ray_x * GRID_STEP
    turn_y = hertz * ray_y * GRID_STEP
    vertical = jnp.full((YTALL, LANES), slow_sq - ray_x * ray_x - ray_y * ray_y, jnp.float32)
    turn_0 = jnp.sqrt(vertical) * (DEPTH_STEP * hertz)
    wave_re = wavelet[0, 0]
    wave_im = wavelet[0, 1]

    block = cols // X_RADIX
    place = lax.broadcasted_iota(jnp.int32, (X_RADIX, cols), 1)
    outer = lax.broadcasted_iota(jnp.int32, (X_RADIX, cols), 0)
    eighth = lax.rem(place * outer, X_RADIX).astype(jnp.float32) * (1.0 / X_RADIX)
    vec_sin, vec_cos = turn_sincos(eighth + place.astype(jnp.float32) * turn_x)
    vecs[0] = vec_cos
    vecs[1] = vec_sin

    width = cols // pieces
    deep = 32

    def x_table(p):
        at = pl.ds(pl.multiple_of(p * width, LANES), width)
        x = lax.broadcasted_iota(jnp.int32, (deep, width), 1) + p * width
        x = x.astype(jnp.float32) * (1.0 / cols)
        k = lax.broadcasted_iota(jnp.int32, (deep, width), 0)

        def strip_of(strip, carry):
            sine, cosine = turn_sincos((k + strip * deep).astype(jnp.float32) * x)
            for k1 in range(X_RADIX):
                vc = vecs[0, k1 : k1 + 1, at]
                vs = vecs[1, k1 : k1 + 1, at]
                row = pl.ds(pl.multiple_of(strip * deep + k1 * block, deep), deep)
                row_im = pl.ds(pl.multiple_of(strip * deep + k1 * block + cols, deep), deep)
                xtab[row, at] = (cosine * vc - sine * vs).astype(jnp.bfloat16)
                xtab[row_im, at] = (-(cosine * vs) - sine * vc).astype(jnp.bfloat16)
            return carry

        lax.fori_loop(0, block // deep, strip_of, 0)

    x_table(0)

    ytiles = short // LANES

    tall = short // YTALL

    def y_table(step, carry):
        n1 = step // (tall * ytiles)
        strip = lax.rem(step // ytiles, tall)
        tile = lax.rem(step, ytiles)
        n2 = lax.broadcasted_iota(jnp.int32, (YTALL, LANES), 0) + strip * YTALL
        k2 = lax.broadcasted_iota(jnp.int32, (YTALL, LANES), 1) + tile * LANES
        n = n2 * radix + n1
        n = n.astype(jnp.float32)
        turns = k2.astype(jnp.float32) * (n * (1.0 / rows))
        turns = turns - jnp.floor(turns)
        sine, cosine = turn_sincos(turns + n * turn_y + turn_0)
        real = (wave_re * cosine + wave_im * sine).astype(jnp.bfloat16)
        imag_f = wave_re * sine - wave_im * cosine
        imag = imag_f.astype(jnp.bfloat16)
        top = pl.ds(pl.multiple_of(strip * YTALL, YTALL), YTALL)
        bottom = pl.ds(pl.multiple_of(strip * YTALL + short, YTALL), YTALL)
        left = pl.ds(pl.multiple_of(tile * LANES, LANES), LANES)
        right = pl.ds(pl.multiple_of(tile * LANES + short, LANES), LANES)
        ytab[n1, top, left] = real
        ytab[n1, top, right] = (-imag_f).astype(jnp.bfloat16)
        ytab[n1, bottom, left] = imag
        ytab[n1, bottom, right] = real
        return carry

    lax.fori_loop(0, radix * tall * ytiles, y_table, 0)

    step_y = 2.0 * math.pi / (rows * GRID_STEP)
    step_x = 2.0 * math.pi / (cols * GRID_STEP)
    imag_sq = imag_arg * imag_arg
    imag_half = imag_arg * 0.5

    sub = lax.broadcasted_iota(jnp.int32, (short, LANES), 0)
    for k1 in range(radix):
        offset = k1 * short - (rows if k1 >= radix // 2 else 0)
        ky = (sub + offset).astype(jnp.float32) * step_y
        ybase[k1] = real_base - ky * ky

    def shift(strip, total):
        load(strip).wait()
        rows_at = pl.ds(pl.multiple_of(strip * 16, 16), 16)

        def inner(tile, acc):
            at = pl.ds(pl.multiple_of(tile * LANES, LANES), LANES)
            kx = lax.broadcasted_iota(jnp.int32, (16, LANES), 1) + tile * LANES
            kx = jnp.where(kx >= cols // 2, kx - cols, kx).astype(jnp.float32) * step_x
            kx_sq = kx * kx
            parts = []
            for k1 in range(radix):
                a = ybase[k1, rows_at, :] - kx_sq
                m = a * a + imag_sq
                q = 0.5 * (m * lax.rsqrt(m) + jnp.abs(a))
                iq = lax.rsqrt(q)
                g = q * iq
                h = imag_half * iq
                forward = a >= 0.0
                vert_re = jnp.where(forward, g, h)
                vert_im = jnp.where(forward, h, g)
                damp = jnp.exp(vert_im * -DEPTH_STEP)
                sine, cosine = half_sincos(
                    vert_re * (0.5 * DEPTH_STEP), PHASE_SIN, PHASE_COS
                )
                cosine = cosine * damp
                sine = sine * damp
                re = spec[0, k1, rows_at, at].astype(jnp.float32)
                im = spec[1, k1, rows_at, at].astype(jnp.float32)
                new_re = re * cosine - im * sine
                new_im = re * sine + im * cosine
                acc = acc + (new_re * new_re + new_im * new_im)
                parts.append((new_re, new_im))
            for n1, (re, im) in enumerate(butterfly(parts)):
                zed[n1, rows_at, at] = re.astype(jnp.bfloat16)
                low = pl.ds(pl.multiple_of(strip * 16 + short, 16), 16)
                zed[n1, low, at] = im.astype(jnp.bfloat16)
            return acc

        return lax.fori_loop(0, tiles, inner, total)

    energy = lax.fori_loop(0, strips, shift, jnp.zeros((16, LANES), jnp.float32))
    etile[...] = energy[:8] + energy[8:]

    chips = groups // 2

    def y_stage(n1, carry):
        for part in range(cols // 256):
            at = slice(part * 256, part * 256 + 256)
            at_im = slice(cols + part * 256, cols + part * 256 + 256)
            res = jnp.dot(ytab[n1], zed[n1, :, at], preferred_element_type=jnp.float32)
            res = res.astype(jnp.bfloat16)
            field[:, n1, :, at] = res[:short].reshape(chips, 16, 256)
            field[:, n1, :, at_im] = res[short:].reshape(chips, 16, 256)
        return carry

    lax.fori_loop(0, radix, y_stage, 0)

    pl.semaphore_wait(barrier, groups - 1)

    def energy_copy(i):
        return pltpu.make_async_remote_copy(
            src_ref=etile, dst_ref=eall.at[i], send_sem=e_s.at[i], recv_sem=e_r.at[i],
            device_id={"freq": lax.rem(me + i, groups)}, device_id_type=MESH,
        )

    def energy_start(i, carry):
        energy_copy(i).start()
        return carry

    lax.fori_loop(1, groups, energy_start, 0)

    def order(j):
        half = j // 2
        return jnp.where(lax.rem(j, 2) == 0, half, lines - 1 - half)

    def cut_of(p):
        return pl.ds(pl.multiple_of(p * width, LANES), width)

    def core_copy(p, b):
        cut = cut_of(p)
        return pltpu.make_async_remote_copy(
            src_ref=image.at[:, b, 1 - core, :, :, cut], dst_ref=core_in.at[:, b, :, :, cut],
            send_sem=core_s.at[p, b], recv_sem=core_r.at[p, b],
            device_id={"freq": core_peer}, device_id_type=MESH,
        )

    def pair_copy(a, p):
        cut = cut_of(p)
        return pltpu.make_async_remote_copy(
            src_ref=image.at[a, 1 - pair, core, :, :, cut], dst_ref=pair_in.at[a, :, :, cut],
            send_sem=pair_s.at[a, p], recv_sem=pair_r.at[a, p],
            device_id={"freq": pair_peer}, device_id_type=MESH,
        )

    def low_copy(a, p):
        cut = cut_of(p)
        return pltpu.make_async_remote_copy(
            src_ref=image.at[a, pair, core, :, :, cut], dst_ref=low_in.at[a, :, :, cut],
            send_sem=low_s.at[a, p], recv_sem=low_r.at[a, p],
            device_id={"freq": jnp.minimum(spot + 1, lines - 1) * 4 + pair * 2 + core},
            device_id_type=MESH,
        )

    def high_copy(a, p):
        cut = cut_of(p)
        return pltpu.make_async_remote_copy(
            src_ref=image.at[a, pair, core, :, :, cut], dst_ref=high_in.at[a, :, :, cut],
            send_sem=high_s.at[a, p], recv_sem=high_r.at[a, p],
            device_id={"freq": jnp.maximum(spot - 1, 0) * 4 + pair * 2 + core},
            device_id_type=MESH,
        )

    count = lines * pieces
    depth = min(DEPTH, count)

    def split(i):
        return order(lax.rem(i, lines)), i // lines

    def first_of(i):
        return lax.rem(i, lines) == 0

    def send_pair(i):
        a, p = split(i)
        cut = cut_of(p)

        @pl.when(first_of(i))
        def _():
            core_copy(p, 1 - pair).wait_recv()

        image[a, 1 - pair, core, :, :, cut] = (
            image[a, 1 - pair, core, :, :, cut] + core_in[a, 1 - pair, :, :, cut]
        )
        pair_copy(a, p).start()

    def third(i, carry):
        @pl.when(i < count)
        def _():
            a, p = split(jnp.minimum(i, count - 1))
            cut = cut_of(p)
            pair_copy(a, p).wait_recv()

            @pl.when(i + depth < count)
            def _():
                send_pair(jnp.minimum(i + depth, count - 1))

            @pl.when(first_of(i))
            def _():
                core_copy(p, pair).wait_recv()

            image[a, pair, core, :, :, cut] = (
                image[a, pair, core, :, :, cut] + core_in[a, pair, :, :, cut] + pair_in[a, :, :, cut]
            )

        upward = i - LAG * spot
        a_up, p_up = split(jnp.clip(upward, 0, count - 1))

        @pl.when((upward >= 0) & (upward < count) & (a_up > spot))
        def _():
            cut = cut_of(p_up)

            @pl.when(spot > 0)
            def _():
                low_copy(a_up, p_up).wait_recv()
                image[a_up, pair, core, :, :, cut] = image[a_up, pair, core, :, :, cut] + low_in[a_up, :, :, cut]

            low_copy(a_up, p_up).start()

        downward = i - LAG * (lines - 1 - spot)
        a_dn, p_dn = split(jnp.clip(downward, 0, count - 1))

        @pl.when((downward >= 0) & (downward < count) & (a_dn < spot))
        def _():
            cut = cut_of(p_dn)

            @pl.when(spot < lines - 1)
            def _():
                high_copy(a_dn, p_dn).wait_recv()
                image[a_dn, pair, core, :, :, cut] = image[a_dn, pair, core, :, :, cut] + high_in[a_dn, :, :, cut]

            high_copy(a_dn, p_dn).start()

        return carry

    def compute(p, carry):
        at = cut_of(p)

        @pl.when(p > 0)
        def _():
            x_table(p)

        @pl.when(p == 1)
        def _():
            lax.fori_loop(0, depth, lambda i, c: (send_pair(i), c)[1], 0)

        lax.fori_loop(EARLY * jnp.maximum(p - 2, 0), EARLY * jnp.maximum(p - 1, 0), third, 0)

        half = max(lines // 4, 1)
        for q in range(lines // half):
            lhs = field[2 * half * q : 2 * half * (q + 1)].reshape(half * 2 * radix * 16, 2 * cols)
            res = jnp.dot(lhs, xtab[:, at], preferred_element_type=jnp.float32)
            res = res.reshape(half, 2, radix, 2, 8, width)
            for c in range(2):
                image[half * q : half * (q + 1), :, c, :, :, at] = res[:, :, :, c]
        core_copy(p, 1 - pair).start()
        core_copy(p, pair).start()
        return carry

    lax.fori_loop(0, pieces, compute, 0)

    lax.fori_loop(EARLY * max(pieces - 2, 0), count + LAG * (lines - 1), third, 0)

    def energy_take(i, total):
        energy_copy(i).wait_recv()
        return total + eall[i]

    total = lax.fori_loop(1, groups, energy_take, etile[...])
    total = jnp.sum(jnp.sum(total, axis=0, keepdims=True), axis=1, keepdims=True)
    scale = lax.rsqrt(total / freq_total + 1e-06)

    def own(p, carry):
        cut = cut_of(p)

        @pl.when(spot > 0)
        def _():
            low_copy(spot, p).wait_recv()
            image[spot, pair, core, :, :, cut] = image[spot, pair, core, :, :, cut] + low_in[spot, :, :, cut]

        @pl.when(spot < lines - 1)
        def _():
            high_copy(spot, p).wait_recv()
            image[spot, pair, core, :, :, cut] = image[spot, pair, core, :, :, cut] + high_in[spot, :, :, cut]

        return carry

    lax.fori_loop(0, pieces, own, 0)
    for n1 in range(radix):
        out_ref[:, n1, :] = image[spot, pair, core, n1] * scale

    def energy_end(i, carry):
        energy_copy(i).wait_send()
        return carry

    lax.fori_loop(1, groups, energy_end, 0)

    def finish_core(p, carry):
        core_copy(p, 0).wait_send()
        core_copy(p, 1).wait_send()
        return carry

    lax.fori_loop(0, pieces, finish_core, 0)

    def finish(a, carry):
        def piece(p, inner):
            pair_copy(a, p).wait_send()

            @pl.when(a > spot)
            def _():
                low_copy(a, p).wait_send()

            @pl.when(a < spot)
            def _():
                high_copy(a, p).wait_send()

            return inner

        return lax.fori_loop(0, pieces, piece, carry)

    lax.fori_loop(0, lines, finish, 0)


def body(spectra, wavelet, freq_index, slowness, layer_ids, ray_slowness):
    slot_total, unused, rows, cols = spectra.shape
    groups = lax.axis_size("freq")
    freq_total = slot_total * groups
    radix = rows // groups // 8
    short = rows // radix
    lines = groups // 4
    pieces = min(4, cols // LANES)
    f32, bf16 = jnp.float32, jnp.bfloat16
    dma = pltpu.SemaphoreType.DMA
    out = pl.pallas_call(
        functools.partial(kernel, groups, radix, pieces, freq_total),
        out_shape=jax.ShapeDtypeStruct((8, radix, cols), f32),
        in_specs=[
            *[pl.BlockSpec(memory_space=pltpu.SMEM)] * 5,
            pl.BlockSpec(memory_space=pl.ANY),
        ],
        out_specs=pl.BlockSpec(memory_space=pltpu.VMEM),
        scratch_shapes=[
            pltpu.VMEM((2, radix, short, cols), bf16),
            pltpu.VMEM((radix, 2 * short, cols), bf16),
            pltpu.VMEM((radix, 2 * short, 2 * short), bf16),
            pltpu.VMEM((groups // 2, radix, 16, 2 * cols), bf16),
            pltpu.VMEM((2 * cols, cols), bf16),
            pltpu.VMEM((2, X_RADIX, cols), f32),
            pltpu.VMEM((radix, short, LANES), f32),
            pltpu.VMEM((lines, 2, 2, radix, 8, cols), f32),
            pltpu.VMEM((lines, 2, radix, 8, cols), f32),
            pltpu.VMEM((lines, radix, 8, cols), f32),
            pltpu.VMEM((lines, radix, 8, cols), f32),
            pltpu.VMEM((lines, radix, 8, cols), f32),
            pltpu.VMEM((8, LANES), f32),
            pltpu.VMEM((groups, 8, LANES), f32),
            dma((short // 16,)),
            dma((pieces, 2)),
            dma((pieces, 2)),
            dma((lines, pieces)),
            dma((lines, pieces)),
            dma((lines, pieces)),
            dma((lines, pieces)),
            dma((lines, pieces)),
            dma((lines, pieces)),
            dma((groups,)),
            dma((groups,)),
        ],
        compiler_params=pltpu.CompilerParams(
            collective_id=0, has_side_effects=True, vmem_limit_bytes=60 * 1024 * 1024
        ),
    )(
        wavelet, freq_index.reshape(1, 1), slowness, layer_ids.reshape(1, 1), ray_slowness,
        spectra.reshape(2, radix, short, cols),
    )
    return out.reshape(1, 8 * radix, cols)


def solution(mesh):
    placed = (
        P(("rays", "freq"), None, None, None),
        P("freq", None),
        P("freq"),
        P(),
        P(),
        P("rays"),
    )
    return jax.shard_map(
        body, mesh=mesh, in_specs=placed, out_specs=P("rays", "freq", None), check_vma=False
    )
```

```python
import functools
import math

import jax
import jax.numpy as jnp
from jax import lax
from jax.experimental import pallas as pl
from jax.experimental.pallas import tpu as pltpu
from jax.sharding import PartitionSpec as P

GRID_STEP = 12.5
DEPTH_STEP = 10.0
LOW_FREQUENCY = 5.0
FREQUENCY_BAND = 50.0
DAMPING = 6.0
X_RADIX = 8
LANES = 128
LAG = 2
DEPTH = 4
YTALL = 64
EARLY = 2
MESH = pl.DeviceIdType.MESH

PHASE_SIN = (0.9999998807907104, -0.16666465997695923, 0.008326363749802113, -0.00019062065985053778)
PHASE_COS = (0.9999992251396179, -0.499982088804245, 0.04160428047180176, -0.0013190462486818433)
TURN_SIN = (0.9999992251396179, -0.16665679216384888, 0.008313224650919437, -0.0001852344867074862)
TURN_COS = (
    0.9999999403953552, -0.4999990463256836, 0.041663579642772675, -0.0013853666605427861,
    2.315317397005856e-05,
)


def polynomial(coefs, square):
    value = square * coefs[-1] + coefs[-2]
    for coef in coefs[-3::-1]:
        value = value * square + coef
    return value


def half_sincos(half, sin_coefs, cos_coefs):
    square = half * half
    sine = polynomial(sin_coefs, square) * half
    twice = sine + sine
    return twice * polynomial(cos_coefs, square), 1.0 - twice * sine


def turn_sincos(turns):
    reduced = turns - jnp.floor(turns + 0.5)
    return half_sincos(reduced * math.pi, TURN_SIN, TURN_COS)


def butterfly(parts):
    count = len(parts)
    if count == 1:
        return parts
    even = butterfly(parts[0::2])
    odd = butterfly(parts[1::2])
    low, high = [], []
    for i in range(count // 2):
        er, ei = even[i]
        xr, xi = odd[i]
        if i == 0:
            tr, ti = xr, xi
        elif 4 * i == count:
            tr, ti = -xi, xr
        elif 8 * i == count:
            root = math.sqrt(0.5)
            tr, ti = (xr - xi) * root, (xr + xi) * root
        elif 8 * i == 3 * count:
            root = math.sqrt(0.5)
            tr, ti = (xr + xi) * -root, (xr - xi) * root
        else:
            c = math.cos(2 * math.pi * i / count)
            s = math.sin(2 * math.pi * i / count)
            tr, ti = xr * c - xi * s, xr * s + xi * c
        low.append((er + tr, ei + ti))
        high.append((er - tr, ei - ti))
    return low + high


def kernel(
    groups, radix, pieces, freq_total,
    wavelet, freq_index, slowness, layer_ids, rays, spec_hbm, out_ref,
    spec, zed, ytab, field, xtab, vecs, ybase, image, core_in, pair_in, low_in, high_in, etile, eall,
    load_sem, core_s, core_r, pair_s, pair_r, low_s, low_r, high_s, high_r, e_s, e_r,
):
    rows = spec.shape[1] * spec.shape[2]
    cols = spec.shape[3]
    short = rows // radix
    lines = groups // 4
    me = lax.axis_index("freq")
    core = lax.rem(me, 2)
    pair = lax.rem(me // 2, 2)
    spot = me // 4
    core_peer = me + 1 - 2 * core
    pair_peer = me + 2 - 4 * pair

    barrier = pltpu.get_barrier_semaphore()

    def greet(i, carry):
        pl.semaphore_signal(
            barrier, inc=1, device_id={"freq": lax.rem(me + i, groups)}, device_id_type=MESH
        )
        return carry

    lax.fori_loop(1, groups, greet, 0)

    strips = short // 16
    tiles = cols // LANES

    def load(i):
        window = pl.ds(pl.multiple_of(i * 16, 16), 16)
        return pltpu.make_async_copy(
            spec_hbm.at[:, :, window, :], spec.at[:, :, window, :], load_sem.at[i]
        )

    def start_load(i, carry):
        load(i).start()
        return carry

    lax.fori_loop(0, strips, start_load, 0)

    hertz = freq_index[0, 0].astype(jnp.float32) * (FREQUENCY_BAND / freq_total) + LOW_FREQUENCY
    angular = hertz * (2.0 * math.pi)
    slow = slowness[layer_ids[0, 0]]
    slow_sq = slow * slow
    ray_x = rays[0]
    ray_y = rays[1]
    real_base = (angular * angular - DAMPING * DAMPING) * slow_sq
    imag_arg = 2.0 * angular * DAMPING * slow_sq
    turn_x = hertz * ray_x * GRID_STEP
    turn_y = hertz * ray_y * GRID_STEP
    vertical = jnp.full((YTALL, LANES), slow_sq - ray_x * ray_x - ray_y * ray_y, jnp.float32)
    turn_0 = jnp.sqrt(vertical) * (DEPTH_STEP * hertz)
    wave_re = wavelet[0, 0]
    wave_im = wavelet[0, 1]

    block = cols // X_RADIX
    place = lax.broadcasted_iota(jnp.int32, (X_RADIX, cols), 1)
    outer = lax.broadcasted_iota(jnp.int32, (X_RADIX, cols), 0)
    eighth = lax.rem(place * outer, X_RADIX).astype(jnp.float32) * (1.0 / X_RADIX)
    vec_sin, vec_cos = turn_sincos(eighth + place.astype(jnp.float32) * turn_x)
    vecs[0] = vec_cos
    vecs[1] = vec_sin

    width = cols // pieces
    deep = 32

    def x_table(p):
        at = pl.ds(pl.multiple_of(p * width, LANES), width)
        x = lax.broadcasted_iota(jnp.int32, (deep, width), 1) + p * width
        x = x.astype(jnp.float32) * (1.0 / cols)
        k = lax.broadcasted_iota(jnp.int32, (deep, width), 0)

        def strip_of(strip, carry):
            sine, cosine = turn_sincos((k + strip * deep).astype(jnp.float32) * x)
            for k1 in range(X_RADIX):
                vc = vecs[0, k1 : k1 + 1, at]
                vs = vecs[1, k1 : k1 + 1, at]
                row = pl.ds(pl.multiple_of(strip * deep + k1 * block, deep), deep)
                row_im = pl.ds(pl.multiple_of(strip * deep + k1 * block + cols, deep), deep)
                xtab[row, at] = (cosine * vc - sine * vs).astype(jnp.bfloat16)
                xtab[row_im, at] = (-(cosine * vs) - sine * vc).astype(jnp.bfloat16)
            return carry

        lax.fori_loop(0, block // deep, strip_of, 0, unroll=True)

    x_table(0)

    ytiles = short // LANES

    tall = short // YTALL

    def y_table(step, carry):
        n1 = step // (tall * ytiles)
        strip = lax.rem(step // ytiles, tall)
        tile = lax.rem(step, ytiles)
        n2 = lax.broadcasted_iota(jnp.int32, (YTALL, LANES), 0) + strip * YTALL
        k2 = lax.broadcasted_iota(jnp.int32, (YTALL, LANES), 1) + tile * LANES
        n = n2 * radix + n1
        n = n.astype(jnp.float32)
        turns = k2.astype(jnp.float32) * (n * (1.0 / rows))
        turns = turns - jnp.floor(turns)
        sine, cosine = turn_sincos(turns + n * turn_y + turn_0)
        real = (wave_re * cosine + wave_im * sine).astype(jnp.bfloat16)
        imag_f = wave_re * sine - wave_im * cosine
        imag = imag_f.astype(jnp.bfloat16)
        top = pl.ds(pl.multiple_of(strip * YTALL, YTALL), YTALL)
        bottom = pl.ds(pl.multiple_of(strip * YTALL + short, YTALL), YTALL)
        left = pl.ds(pl.multiple_of(tile * LANES, LANES), LANES)
        right = pl.ds(pl.multiple_of(tile * LANES + short, LANES), LANES)
        ytab[n1, top, left] = real
        ytab[n1, top, right] = (-imag_f).astype(jnp.bfloat16)
        ytab[n1, bottom, left] = imag
        ytab[n1, bottom, right] = real
        return carry

    lax.fori_loop(0, radix * tall * ytiles, y_table, 0, unroll=2)

    step_y = 2.0 * math.pi / (rows * GRID_STEP)
    step_x = 2.0 * math.pi / (cols * GRID_STEP)
    imag_sq = imag_arg * imag_arg
    imag_half = imag_arg * 0.5

    sub = lax.broadcasted_iota(jnp.int32, (short, LANES), 0)
    for k1 in range(radix):
        offset = k1 * short - (rows if k1 >= radix // 2 else 0)
        ky = (sub + offset).astype(jnp.float32) * step_y
        ybase[k1] = real_base - ky * ky

    def shift(strip, total):
        load(strip).wait()
        rows_at = pl.ds(pl.multiple_of(strip * 16, 16), 16)

        def inner(tile, acc):
            at = pl.ds(pl.multiple_of(tile * LANES, LANES), LANES)
            kx = lax.broadcasted_iota(jnp.int32, (16, LANES), 1) + tile * LANES
            kx = jnp.where(kx >= cols // 2, kx - cols, kx).astype(jnp.float32) * step_x
            kx_sq = kx * kx
            parts = []
            for k1 in range(radix):
                a = ybase[k1, rows_at, :] - kx_sq
                m = a * a + imag_sq
                q = 0.5 * (m * lax.rsqrt(m) + jnp.abs(a))
                iq = lax.rsqrt(q)
                g = q * iq
                h = imag_half * iq
                forward = a >= 0.0
                vert_re = jnp.where(forward, g, h)
                vert_im = jnp.where(forward, h, g)
                damp = jnp.exp(vert_im * -DEPTH_STEP)
                sine, cosine = half_sincos(
                    vert_re * (0.5 * DEPTH_STEP), PHASE_SIN, PHASE_COS
                )
                cosine = cosine * damp
                sine = sine * damp
                re = spec[0, k1, rows_at, at].astype(jnp.float32)
                im = spec[1, k1, rows_at, at].astype(jnp.float32)
                new_re = re * cosine - im * sine
                new_im = re * sine + im * cosine
                acc = acc + (new_re * new_re + new_im * new_im)
                parts.append((new_re, new_im))
            for n1, (re, im) in enumerate(butterfly(parts)):
                zed[n1, rows_at, at] = re.astype(jnp.bfloat16)
                low = pl.ds(pl.multiple_of(strip * 16 + short, 16), 16)
                zed[n1, low, at] = im.astype(jnp.bfloat16)
            return acc

        return lax.fori_loop(0, tiles, inner, total, unroll=2)

    energy = lax.fori_loop(0, strips, shift, jnp.zeros((16, LANES), jnp.float32))
    etile[...] = energy[:8] + energy[8:]

    chips = groups // 2

    def y_stage(n1, carry):
        for part in range(cols // 256):
            at = slice(part * 256, part * 256 + 256)
            at_im = slice(cols + part * 256, cols + part * 256 + 256)
            res = jnp.dot(ytab[n1], zed[n1, :, at], preferred_element_type=jnp.float32)
            res = res.astype(jnp.bfloat16)
            field[:, n1, :, at] = res[:short].reshape(chips, 16, 256)
            field[:, n1, :, at_im] = res[short:].reshape(chips, 16, 256)
        return carry

    lax.fori_loop(0, radix, y_stage, 0, unroll=True)

    pl.semaphore_wait(barrier, groups - 1)

    def energy_copy(i):
        return pltpu.make_async_remote_copy(
            src_ref=etile, dst_ref=eall.at[i], send_sem=e_s.at[i], recv_sem=e_r.at[i],
            device_id={"freq": lax.rem(me + i, groups)}, device_id_type=MESH,
        )

    def energy_start(i, carry):
        energy_copy(i).start()
        return carry

    lax.fori_loop(1, groups, energy_start, 0)

    def order(j):
        half = j // 2
        return jnp.where(lax.rem(j, 2) == 0, half, lines - 1 - half)

    def cut_of(p):
        return pl.ds(pl.multiple_of(p * width, LANES), width)

    def core_copy(p, b):
        cut = cut_of(p)
        return pltpu.make_async_remote_copy(
            src_ref=image.at[:, b, 1 - core, :, :, cut], dst_ref=core_in.at[:, b, :, :, cut],
            send_sem=core_s.at[p, b], recv_sem=core_r.at[p, b],
            device_id={"freq": core_peer}, device_id_type=MESH,
        )

    def pair_copy(a, p):
        cut = cut_of(p)
        return pltpu.make_async_remote_copy(
            src_ref=image.at[a, 1 - pair, core, :, :, cut], dst_ref=pair_in.at[a, :, :, cut],
            send_sem=pair_s.at[a, p], recv_sem=pair_r.at[a, p],
            device_id={"freq": pair_peer}, device_id_type=MESH,
        )

    def low_copy(a, p):
        cut = cut_of(p)
        return pltpu.make_async_remote_copy(
            src_ref=image.at[a, pair, core, :, :, cut], dst_ref=low_in.at[a, :, :, cut],
            send_sem=low_s.at[a, p], recv_sem=low_r.at[a, p],
            device_id={"freq": jnp.minimum(spot + 1, lines - 1) * 4 + pair * 2 + core},
            device_id_type=MESH,
        )

    def high_copy(a, p):
        cut = cut_of(p)
        return pltpu.make_async_remote_copy(
            src_ref=image.at[a, pair, core, :, :, cut], dst_ref=high_in.at[a, :, :, cut],
            send_sem=high_s.at[a, p], recv_sem=high_r.at[a, p],
            device_id={"freq": jnp.maximum(spot - 1, 0) * 4 + pair * 2 + core},
            device_id_type=MESH,
        )

    count = lines * pieces
    depth = min(DEPTH, count)

    def split(i):
        return order(lax.rem(i, lines)), i // lines

    def first_of(i):
        return lax.rem(i, lines) == 0

    def send_pair(i):
        a, p = split(i)
        cut = cut_of(p)

        @pl.when(first_of(i))
        def _():
            core_copy(p, 1 - pair).wait_recv()

        image[a, 1 - pair, core, :, :, cut] = (
            image[a, 1 - pair, core, :, :, cut] + core_in[a, 1 - pair, :, :, cut]
        )
        pair_copy(a, p).start()

    def third(i, carry):
        @pl.when(i < count)
        def _():
            a, p = split(jnp.minimum(i, count - 1))
            cut = cut_of(p)
            pair_copy(a, p).wait_recv()

            @pl.when(i + depth < count)
            def _():
                send_pair(jnp.minimum(i + depth, count - 1))

            @pl.when(first_of(i))
            def _():
                core_copy(p, pair).wait_recv()

            image[a, pair, core, :, :, cut] = (
                image[a, pair, core, :, :, cut] + core_in[a, pair, :, :, cut] + pair_in[a, :, :, cut]
            )

        upward = i - LAG * spot
        a_up, p_up = split(jnp.clip(upward, 0, count - 1))

        @pl.when((upward >= 0) & (upward < count) & (a_up > spot))
        def _():
            cut = cut_of(p_up)

            @pl.when(spot > 0)
            def _():
                low_copy(a_up, p_up).wait_recv()
                image[a_up, pair, core, :, :, cut] = image[a_up, pair, core, :, :, cut] + low_in[a_up, :, :, cut]

            low_copy(a_up, p_up).start()

        downward = i - LAG * (lines - 1 - spot)
        a_dn, p_dn = split(jnp.clip(downward, 0, count - 1))

        @pl.when((downward >= 0) & (downward < count) & (a_dn < spot))
        def _():
            cut = cut_of(p_dn)

            @pl.when(spot < lines - 1)
            def _():
                high_copy(a_dn, p_dn).wait_recv()
                image[a_dn, pair, core, :, :, cut] = image[a_dn, pair, core, :, :, cut] + high_in[a_dn, :, :, cut]

            high_copy(a_dn, p_dn).start()

        return carry

    def compute(p, carry):
        at = cut_of(p)

        @pl.when(p > 0)
        def _():
            x_table(p)

        @pl.when(p == 1)
        def _():
            lax.fori_loop(0, depth, lambda i, c: (send_pair(i), c)[1], 0)

        lax.fori_loop(EARLY * jnp.maximum(p - 2, 0), EARLY * jnp.maximum(p - 1, 0), third, 0)

        half = max(lines // 4, 1)
        for q in range(lines // half):
            lhs = field[2 * half * q : 2 * half * (q + 1)].reshape(half * 2 * radix * 16, 2 * cols)
            res = jnp.dot(lhs, xtab[:, at], preferred_element_type=jnp.float32)
            res = res.reshape(half, 2, radix, 2, 8, width)
            for c in range(2):
                image[half * q : half * (q + 1), :, c, :, :, at] = res[:, :, :, c]
        core_copy(p, 1 - pair).start()
        core_copy(p, pair).start()
        return carry

    lax.fori_loop(0, pieces, compute, 0)

    lax.fori_loop(EARLY * max(pieces - 2, 0), count + LAG * (lines - 1), third, 0)

    def energy_take(i, total):
        energy_copy(i).wait_recv()
        return total + eall[i]

    total = lax.fori_loop(1, groups, energy_take, etile[...])
    total = jnp.sum(jnp.sum(total, axis=0, keepdims=True), axis=1, keepdims=True)
    scale = lax.rsqrt(total / freq_total + 1e-06)

    def own(p, carry):
        cut = cut_of(p)

        @pl.when(spot > 0)
        def _():
            low_copy(spot, p).wait_recv()
            image[spot, pair, core, :, :, cut] = image[spot, pair, core, :, :, cut] + low_in[spot, :, :, cut]

        @pl.when(spot < lines - 1)
        def _():
            high_copy(spot, p).wait_recv()
            image[spot, pair, core, :, :, cut] = image[spot, pair, core, :, :, cut] + high_in[spot, :, :, cut]

        return carry

    lax.fori_loop(0, pieces, own, 0)
    for n1 in range(radix):
        out_ref[:, n1, :] = image[spot, pair, core, n1] * scale

    def energy_end(i, carry):
        energy_copy(i).wait_send()
        return carry

    lax.fori_loop(1, groups, energy_end, 0)

    def finish_core(p, carry):
        core_copy(p, 0).wait_send()
        core_copy(p, 1).wait_send()
        return carry

    lax.fori_loop(0, pieces, finish_core, 0)

    def finish(a, carry):
        def piece(p, inner):
            pair_copy(a, p).wait_send()

            @pl.when(a > spot)
            def _():
                low_copy(a, p).wait_send()

            @pl.when(a < spot)
            def _():
                high_copy(a, p).wait_send()

            return inner

        return lax.fori_loop(0, pieces, piece, carry)

    lax.fori_loop(0, lines, finish, 0)


def body(spectra, wavelet, freq_index, slowness, layer_ids, ray_slowness):
    slot_total, unused, rows, cols = spectra.shape
    groups = lax.axis_size("freq")
    freq_total = slot_total * groups
    radix = rows // groups // 8
    short = rows // radix
    lines = groups // 4
    pieces = min(4, cols // LANES)
    f32, bf16 = jnp.float32, jnp.bfloat16
    dma = pltpu.SemaphoreType.DMA
    out = pl.pallas_call(
        functools.partial(kernel, groups, radix, pieces, freq_total),
        out_shape=jax.ShapeDtypeStruct((8, radix, cols), f32),
        in_specs=[
            *[pl.BlockSpec(memory_space=pltpu.SMEM)] * 5,
            pl.BlockSpec(memory_space=pl.ANY),
        ],
        out_specs=pl.BlockSpec(memory_space=pltpu.VMEM),
        scratch_shapes=[
            pltpu.VMEM((2, radix, short, cols), bf16),
            pltpu.VMEM((radix, 2 * short, cols), bf16),
            pltpu.VMEM((radix, 2 * short, 2 * short), bf16),
            pltpu.VMEM((groups // 2, radix, 16, 2 * cols), bf16),
            pltpu.VMEM((2 * cols, cols), bf16),
            pltpu.VMEM((2, X_RADIX, cols), f32),
            pltpu.VMEM((radix, short, LANES), f32),
            pltpu.VMEM((lines, 2, 2, radix, 8, cols), f32),
            pltpu.VMEM((lines, 2, radix, 8, cols), f32),
            pltpu.VMEM((lines, radix, 8, cols), f32),
            pltpu.VMEM((lines, radix, 8, cols), f32),
            pltpu.VMEM((lines, radix, 8, cols), f32),
            pltpu.VMEM((8, LANES), f32),
            pltpu.VMEM((groups, 8, LANES), f32),
            dma((short // 16,)),
            dma((pieces, 2)),
            dma((pieces, 2)),
            dma((lines, pieces)),
            dma((lines, pieces)),
            dma((lines, pieces)),
            dma((lines, pieces)),
            dma((lines, pieces)),
            dma((lines, pieces)),
            dma((groups,)),
            dma((groups,)),
        ],
        compiler_params=pltpu.CompilerParams(
            collective_id=0, has_side_effects=True, vmem_limit_bytes=60 * 1024 * 1024
        ),
    )(
        wavelet, freq_index.reshape(1, 1), slowness, layer_ids.reshape(1, 1), ray_slowness,
        spectra.reshape(2, radix, short, cols),
    )
    return out.reshape(1, 8 * radix, cols)


def solution(mesh):
    placed = (
        P(("rays", "freq"), None, None, None),
        P("freq", None),
        P("freq"),
        P(),
        P(),
        P("rays"),
    )
    return jax.shard_map(
        body, mesh=mesh, in_specs=placed, out_specs=P("rays", "freq", None), check_vma=False
    )
```
